32 devices in a mesh: rows: 4 (over z), tp: 4 (over y, x), unit: 2 (over core).
Axes of the slice: x: 2, y: 2, z: 4, core: 2. Of those that a mesh axis runs over, the one named last changes fastest.
Arguments:
- train_query: bfloat16 [4096, 2048], P(('unit', 'rows'), 'tp'), parts along dimension 0, may hold values from -0.125 to 0.125
- low_query: bfloat16 [4096, 64], P(('unit', 'rows')), parts along dimension 0, may hold values from -0.125 to 0.125
- high_query: bfloat16 [128, 2048], P('unit', 'tp'), parts along dimension 0, may hold values from -0.75 to 0.75
- train_key: bfloat16 [4096, 512], P(('unit', 'rows'), 'tp'), parts along dimension 0, may hold values from -0.125 to 0.125
- low_key: bfloat16 [4096, 64], P(('unit', 'rows')), parts along dimension 0, may hold values from -0.125 to 0.125
- high_key: bfloat16 [128, 512], P('unit', 'tp'), parts along dimension 0, may hold values from -0.75 to 0.75
- train_value: bfloat16 [4096, 512], P(('unit', 'rows'), 'tp'), parts along dimension 0, may hold values from -0.125 to 0.125
- low_value: bfloat16 [4096, 64], P(('unit', 'rows')), parts along dimension 0, may hold values from -0.125 to 0.125
- high_value: bfloat16 [128, 512], P('unit', 'tp'), parts along dimension 0, may hold values from -0.75 to 0.75
- norm_train: float32 [4096], P(('unit', 'rows', 'tp')), parts along dimension 0, may hold values from 0.25 to 1.75
- norm_step: float32 [4096], P(('unit', 'rows', 'tp')), parts along dimension 0, may hold values from -0.3 to 0.3
Outputs:
- final_query: bfloat16 [4096, 2048], P(('unit', 'tp')), parts along dimension 0
- final_key: bfloat16 [1024, 2048], P(('unit', 'tp')), parts along dimension 0
- final_value: bfloat16 [1024, 2048], P(('unit', 'tp')), parts along dimension 0
- serve_norm: bfloat16 [4096], P('unit'), parts along dimension 0
The draws below stay inside these ranges and needn't reach their ends.
There are 2 independent parts, one for each index of `unit`. The reference program is written for one: setup_inputs(seed, part) draws one part's arguments, and reference() takes and returns one part's arrays. A program takes and returns all parts, laid end to end along the dimension named above; each array names one. Nothing has to cross between parts.
All inputs are finite; a program needn't handle non-finite values.
Results may differ from the reference program's by a relative error of at most 0.001.
Values may be sent and summed in bfloat16 or wider, within the bound.
A program may use at most 64 MiB of HBM per device.

```python
import jax
import jax.numpy as jnp

D_MODEL = 2048
Q_DIM = 2048
KV_DIM = 512
RANK = 64


def block_levels(key, dims, split, least, largest):
    def one(axis_at, blocks):
        heights = jax.random.uniform(jax.random.fold_in(jax.random.fold_in(key, 6), axis_at), (blocks,), jnp.float32, least / len(split), largest / len(split))
        return jnp.repeat(jnp.exp(heights), dims[axis_at] // blocks).reshape((-1,) + (1,) * (len(dims) - axis_at - 1))

    gain = one(*split[0])
    for cut in split[1:]:
        gain = gain * one(*cut)
    return gain


def scatter_about(key, shape, scale, bound, cuts=(), kind=jnp.bfloat16):
    result = jax.random.normal(key, shape, jnp.float32) * scale
    if len(cuts) > 0:
        result = block_levels(key, shape, cuts, -0.22, 0.18) * result
    return jnp.clip(result, min=-bound, max=bound).astype(kind)


def setup_inputs(seed: int = 0, part: int = 0) -> dict:
    streams_of = jax.random.split(jax.random.key(seed), 12)
    own_keys = jax.random.split(jax.random.fold_in(streams_of[11], part), 12)
    return {
        "train_query": scatter_about(own_keys[0], (D_MODEL, Q_DIM), D_MODEL ** -0.5, 0.125, ((0, 4), (1, 4))),
        "low_query": scatter_about(own_keys[1], (D_MODEL, RANK), D_MODEL ** -0.5, 0.125, ((0, 4),)),
        "high_query": scatter_about(own_keys[2], (RANK, Q_DIM), RANK ** -0.5, 0.75, ((1, 4),)),
        "train_key": scatter_about(own_keys[3], (D_MODEL, KV_DIM), D_MODEL ** -0.5, 0.125, ((0, 4), (1, 4))),
        "low_key": scatter_about(own_keys[4], (D_MODEL, RANK), D_MODEL ** -0.5, 0.125, ((0, 4),)),
        "high_key": scatter_about(own_keys[5], (RANK, KV_DIM), RANK ** -0.5, 0.75, ((1, 4),)),
        "train_value": scatter_about(own_keys[6], (D_MODEL, KV_DIM), D_MODEL ** -0.5, 0.125, ((0, 4), (1, 4))),
        "low_value": scatter_about(own_keys[7], (D_MODEL, RANK), D_MODEL ** -0.5, 0.125, ((0, 4),)),
        "high_value": scatter_about(own_keys[8], (RANK, KV_DIM), RANK ** -0.5, 0.75, ((1, 4),)),
        "norm_train": jnp.clip(1.0 + 0.15 * jax.random.normal(own_keys[9], (D_MODEL,), jnp.float32), 0.25, 1.75),
        "norm_step": jnp.clip(jax.random.uniform(own_keys[10], (D_MODEL,), jnp.float32, -0.3, 0.3) * block_levels(own_keys[10], (D_MODEL,), ((0, 16),), -0.4, 0.0), -0.3, 0.3),
    }


mix_rate = 0.5


def reference(train_query, low_query, high_query, train_key, low_key, high_key, train_value, low_value, high_value, norm_train, norm_step):
    result_query = train_query.astype(jnp.float32) + mix_rate * jnp.dot(low_query, high_query, preferred_element_type=jnp.float32)
    result_key = train_key.astype(jnp.float32) + mix_rate * jnp.dot(low_key, high_key, preferred_element_type=jnp.float32)
    result_value = train_value.astype(jnp.float32) + mix_rate * jnp.dot(low_value, high_value, preferred_element_type=jnp.float32)
    final_query = result_query.T.astype(jnp.bfloat16)
    final_key = result_key.T.astype(jnp.bfloat16)
    final_value = result_value.T.astype(jnp.bfloat16)
    serve_norm = (norm_train + norm_step).astype(jnp.bfloat16)
    return final_query, final_key, final_value, serve_norm
```

```python
import functools

import jax
import jax.numpy as jnp
from jax import lax
from jax.experimental import pallas as pl
from jax.experimental.pallas import tpu as pltpu
from jax.sharding import PartitionSpec as P

mix_rate = 0.5
MESH = pl.DeviceIdType.MESH
LANES = 128


def kernel(
    n,
    peers,
    rows,
    *refs,
):
    (tq, lq, hq, tk, lk, hk, tv, lv, hv, norm_train, norm_step) = refs[:11]
    (oq, ok, ov, out_norm) = refs[11:15]
    held = refs[15:26]
    (gains, in_sem, send_sem, recv_sem, peer_send, peer_recv) = refs[26:]
    outs = (oq, ok, ov)
    me, part = lax.axis_index("rows"), lax.axis_index("tp")
    right, left = lax.rem(me + 1, n), lax.rem(me + n - 1, n)
    has_right, has_left = me < n - 1, me > 0

    barrier = pltpu.get_barrier_semaphore()

    def greet(axis, index):
        pl.semaphore_signal(barrier, inc=1, device_id={axis: index}, device_id_type=MESH)

    loads = [
        pltpu.make_async_copy(source, target, in_sem.at[i])
        for i, (source, target) in enumerate(zip(refs[:11], held))
    ]

    @pl.when(has_right)
    def _():
        greet("rows", right)

    @pl.when(has_left)
    def _():
        greet("rows", left)

    for step in range(1, peers):
        greet("tp", lax.rem(part + step, peers))
    for i in (1, 2, 0, 4, 5, 3, 7, 8, 6, 9, 10):
        loads[i].start()

    pieces = []
    for which, out in enumerate(outs):
        height = out.shape[-2]
        width = LANES if height % LANES == 0 else height
        pieces += [(which, start, width) for start in range(0, height, width)]
    norm_piece = len(pieces)

    def view(c, k):
        if c == norm_piece:
            return gains.at[k]
        which, start, width = pieces[c]
        out = outs[which]
        if len(out.shape) == 3:
            return out.at[k, pl.ds(start, width), :]
        return out.at[pl.ds(start, width), pl.ds(pl.multiple_of(k * rows, rows), rows)]

    def hop(c, k, way):
        return pltpu.make_async_remote_copy(
            src_ref=view(c, k),
            dst_ref=view(c, k),
            send_sem=send_sem.at[way, k, c],
            recv_sem=recv_sem.at[k, c],
            device_id={"rows": left if way else right},
            device_id_type=MESH,
        )

    def both_ways(c):
        @pl.when(has_right)
        def _():
            hop(c, me, 0).start()

        @pl.when(has_left)
        def _():
            hop(c, me, 1).start()

    ready = set()

    def merge(c):
        which, start, width = pieces[c]
        train, low, high = held[3 * which : 3 * which + 3]
        if which not in ready:
            ready.add(which)
            for i in (1, 2, 0):
                loads[3 * which + i].wait()
        span = pl.ds(start, width)
        product = lax.dot_general(
            high[:, span], low[...], (((0,), (0,)), ((), ())), preferred_element_type=jnp.float32
        )
        result = train[:, span].T.astype(jnp.float32) + mix_rate * product
        view(c, me)[...] = result.astype(jnp.bfloat16)

    merge(0)
    merge(1)
    pl.semaphore_wait(
        barrier, peers - 1 + has_right.astype(jnp.int32) + has_left.astype(jnp.int32)
    )
    both_ways(0)
    for c in range(2, norm_piece):
        merge(c)
        both_ways(c - 1)
    loads[9].wait()
    loads[10].wait()
    gains[me, part] = held[9][...] + held[10][...]
    both_ways(norm_piece - 1)

    def to_peer(step):
        return pltpu.make_async_remote_copy(
            src_ref=gains.at[me, part],
            dst_ref=gains.at[me, part],
            send_sem=peer_send.at[step],
            recv_sem=peer_recv.at[step],
            device_id={"tp": lax.rem(part + step, peers)},
            device_id_type=MESH,
        )

    for step in range(1, peers):
        to_peer(step).start()
    for step in range(1, peers):
        to_peer(step).wait()
    both_ways(norm_piece)

    def pass_on(step, carry):
        for c in range(norm_piece + 1):

            @pl.when(me - step >= 0)
            def _():
                hop(c, me - step, 0).wait_recv()

                @pl.when(has_right)
                def _():
                    hop(c, me - step, 0).start()

            @pl.when(me + step < n)
            def _():
                hop(c, me + step, 1).wait_recv()

                @pl.when(has_left)
                def _():
                    hop(c, me + step, 1).start()

        return carry

    lax.fori_loop(1, n, pass_on, 0)
    for k in range(n):
        for t in range(peers):
            out_norm[k * peers + t : k * peers + t + 1, :] = gains[k, t]

    def sent(step, carry):
        for c in range(norm_piece + 1):

            @pl.when((me - step >= 0) & has_right)
            def _():
                hop(c, me - step, 0).wait_send()

            @pl.when((me + step < n) & has_left)
            def _():
                hop(c, me + step, 1).wait_send()

        return carry

    lax.fori_loop(0, n, sent, 0)


def solution(mesh):
    n, peers = mesh.shape["rows"], mesh.shape["tp"]

    def shards(tq, lq, hq, tk, lk, hk, tv, lv, hv, norm_train, norm_step):
        rows = tq.shape[0]
        whole_tiles = rows % LANES == 0
        trains = (tq, tk, tv)
        operands = (
            tq, lq.T, hq, tk, lk.T, hk, tv, lv.T, hv,
            norm_train.reshape(1, -1), norm_step.reshape(1, -1),
        )
        heights = [train.shape[1] for train in trains]
        shapes = [
            (height, n * rows) if whole_tiles else (n, height, rows) for height in heights
        ]
        pieces = 1 + sum(h // LANES if h % LANES == 0 else 1 for h in heights)
        width = norm_train.shape[0]
        outs = pl.pallas_call(
            functools.partial(kernel, n, peers, rows),
            out_shape=[jax.ShapeDtypeStruct(shape, jnp.bfloat16) for shape in shapes]
            + [jax.ShapeDtypeStruct((n * peers, width), jnp.float32)],
            in_specs=[pl.BlockSpec(memory_space=pl.ANY)] * len(operands),
            out_specs=[pl.BlockSpec(memory_space=pltpu.VMEM)] * 4,
            scratch_shapes=[pltpu.VMEM(x.shape, x.dtype) for x in operands]
            + [
                pltpu.VMEM((n, peers, 1, width), jnp.float32),
                pltpu.SemaphoreType.DMA((len(operands),)),
                pltpu.SemaphoreType.DMA((2, n, pieces)),
                pltpu.SemaphoreType.DMA((n, pieces)),
                pltpu.SemaphoreType.DMA((peers,)),
                pltpu.SemaphoreType.DMA((peers,)),
            ],
            compiler_params=pltpu.CompilerParams(collective_id=0, has_side_effects=True),
        )(*operands)
        finals = [
            out if whole_tiles else out.transpose(1, 0, 2).reshape(height, n * rows)
            for out, height in zip(outs, heights)
        ]
        return (*finals, outs[3].astype(jnp.bfloat16).reshape(-1))

    in_specs = (
        P(("unit", "rows"), "tp"),
        P(("unit", "rows"), None),
        P("unit", "tp"),
    ) * 3 + (P(("unit", "rows", "tp")),) * 2
    out_specs = (P(("unit", "tp"), None),) * 3 + (P("unit"),)
    return jax.shard_map(shards, mesh=mesh, in_specs=in_specs, out_specs=out_specs, check_vma=False)
```

```python
import functools

import jax
import jax.numpy as jnp
from jax import lax
from jax.experimental import pallas as pl
from jax.experimental.pallas import tpu as pltpu
from jax.sharding import PartitionSpec as P

mix_rate = 0.5
MESH = pl.DeviceIdType.MESH
LANES = 128


def kernel(
    n,
    peers,
    rows,
    *refs,
):
    (tq, lq, hq, tk, lk, hk, tv, lv, hv, norm_train, norm_step) = refs[:11]
    (oq, ok, ov, out_norm) = refs[11:15]
    held = refs[15:26]
    (gains, in_sem, send_sem, recv_sem, peer_send, peer_recv) = refs[26:]
    outs = (oq, ok, ov)
    me, part = lax.axis_index("rows"), lax.axis_index("tp")
    right, left = lax.rem(me + 1, n), lax.rem(me + n - 1, n)
    has_right, has_left = me < n - 1, me > 0

    barrier = pltpu.get_barrier_semaphore()

    def greet(axis, index):
        pl.semaphore_signal(barrier, inc=1, device_id={axis: index}, device_id_type=MESH)

    loads = [
        pltpu.make_async_copy(source, target, in_sem.at[i])
        for i, (source, target) in enumerate(zip(refs[:11], held))
    ]

    @pl.when(has_right)
    def _():
        greet("rows", right)

    @pl.when(has_left)
    def _():
        greet("rows", left)

    for step in range(1, peers):
        greet("tp", lax.rem(part + step, peers))
    for i in (1, 2, 0, 4, 5, 3, 7, 8, 6, 9, 10):
        loads[i].start()

    pieces = []
    for which, out in enumerate(outs):
        height = out.shape[-2]
        width = LANES if height % LANES == 0 else height
        pieces += [(which, start, width) for start in range(0, height, width)]
    norm_piece = len(pieces)

    def view(c, k):
        if c == norm_piece:
            return gains.at[k]
        which, start, width = pieces[c]
        out = outs[which]
        if len(out.shape) == 3:
            return out.at[k, pl.ds(start, width), :]
        return out.at[pl.ds(start, width), pl.ds(pl.multiple_of(k * rows, rows), rows)]

    def hop(c, k, way):
        return pltpu.make_async_remote_copy(
            src_ref=view(c, k),
            dst_ref=view(c, k),
            send_sem=send_sem.at[way, k, c],
            recv_sem=recv_sem.at[k, c],
            device_id={"rows": left if way else right},
            device_id_type=MESH,
        )

    def both_ways(c):
        @pl.when(has_right)
        def _():
            hop(c, me, 0).start()

        @pl.when(has_left)
        def _():
            hop(c, me, 1).start()

    ready = set()

    def merge(c):
        which, start, width = pieces[c]
        train, low, high = held[3 * which : 3 * which + 3]
        if which not in ready:
            ready.add(which)
            for i in (1, 2, 0):
                loads[3 * which + i].wait()
        span = pl.ds(start, width)
        product = lax.dot_general(
            high[:, span], low[...], (((0,), (0,)), ((), ())), preferred_element_type=jnp.float32
        )
        result = train[:, span].T.astype(jnp.float32) + mix_rate * product
        view(c, me)[...] = result.astype(jnp.bfloat16)

    merge(0)
    merge(1)
    pl.semaphore_wait(
        barrier, peers - 1 + has_right.astype(jnp.int32) + has_left.astype(jnp.int32)
    )
    both_ways(0)
    for c in range(2, norm_piece):
        merge(c)
        both_ways(c - 1)
    loads[9].wait()
    loads[10].wait()
    gains[me, part] = held[9][...] + held[10][...]
    both_ways(norm_piece - 1)

    def to_peer(step):
        return pltpu.make_async_remote_copy(
            src_ref=gains.at[me, part],
            dst_ref=gains.at[me, part],
            send_sem=peer_send.at[step],
            recv_sem=peer_recv.at[step],
            device_id={"tp": lax.rem(part + step, peers)},
            device_id_type=MESH,
        )

    for step in range(1, peers):
        to_peer(step).start()
    for step in range(1, peers):
        to_peer(step).wait()
    both_ways(norm_piece)

    def pass_on(step, carry):
        for c in range(norm_piece + 1):

            @pl.when(me - step >= 0)
            def _():
                hop(c, me - step, 0).wait_recv()

                @pl.when(has_right)
                def _():
                    hop(c, me - step, 0).start()

            @pl.when(me + step < n)
            def _():
                hop(c, me + step, 1).wait_recv()

                @pl.when(has_left)
                def _():
                    hop(c, me + step, 1).start()

        return carry

    lax.fori_loop(1, n, pass_on, 0)
    for k in range(n):
        for t in range(peers):
            out_norm[k * peers + t : k * peers + t + 1, :] = gains[k, t]

    def sent(step, carry):
        for c in range(norm_piece + 1):

            @pl.when((me - step >= 0) & has_right)
            def _():
                hop(c, me - step, 0).wait_send()

            @pl.when((me + step < n) & has_left)
            def _():
                hop(c, me + step, 1).wait_send()

        return carry

    lax.fori_loop(0, n, sent, 0)


def solution(mesh):
    n, peers = mesh.shape["rows"], mesh.shape["tp"]

    def shards(tq, lq, hq, tk, lk, hk, tv, lv, hv, norm_train, norm_step):
        rows = tq.shape[0]
        whole_tiles = rows % LANES == 0
        trains = (tq, tk, tv)
        operands = (
            tq, lq.T, hq, tk, lk.T, hk, tv, lv.T, hv,
            norm_train.reshape(1, -1), norm_step.reshape(1, -1),
        )
        heights = [train.shape[1] for train in trains]
        shapes = [
            (height, n * rows) if whole_tiles else (n, height, rows) for height in heights
        ]
        pieces = 1 + sum(h // LANES if h % LANES == 0 else 1 for h in heights)
        width = norm_train.shape[0]
        outs = pl.pallas_call(
            functools.partial(kernel, n, peers, rows),
            out_shape=[
                (pltpu.VMEM if whole_tiles else jax.ShapeDtypeStruct)(shape, jnp.bfloat16)
                for shape in shapes
            ]
            + [jax.ShapeDtypeStruct((n * peers, width), jnp.float32)],
            in_specs=[pl.BlockSpec(memory_space=pl.ANY)] * len(operands),
            out_specs=[pl.BlockSpec(memory_space=pltpu.VMEM)] * 4,
            scratch_shapes=[pltpu.VMEM(x.shape, x.dtype) for x in operands]
            + [
                pltpu.VMEM((n, peers, 1, width), jnp.float32),
                pltpu.SemaphoreType.DMA((len(operands),)),
                pltpu.SemaphoreType.DMA((2, n, pieces)),
                pltpu.SemaphoreType.DMA((n, pieces)),
                pltpu.SemaphoreType.DMA((peers,)),
                pltpu.SemaphoreType.DMA((peers,)),
            ],
            compiler_params=pltpu.CompilerParams(collective_id=0, has_side_effects=True),
        )(*operands)
        finals = [
            out if whole_tiles else out.transpose(1, 0, 2).reshape(height, n * rows)
            for out, height in zip(outs, heights)
        ]
        return (*finals, outs[3].astype(jnp.bfloat16).reshape(-1))

    in_specs = (
        P(("unit", "rows"), "tp"),
        P(("unit", "rows"), None),
        P("unit", "tp"),
    ) * 3 + (P(("unit", "rows", "tp")),) * 2
    out_specs = (P(("unit", "tp"), None),) * 3 + (P("unit"),)
    return jax.shard_map(shards, mesh=mesh, in_specs=in_specs, out_specs=out_specs, check_vma=False)
```

```python
import functools

import jax
import jax.numpy as jnp
from jax import lax
from jax.experimental import pallas as pl
from jax.experimental.pallas import tpu as pltpu
from jax.sharding import PartitionSpec as P

mix_rate = 0.5
MESH = pl.DeviceIdType.MESH
LANES = 128


def kernel(
    n,
    peers,
    rows,
    *refs,
):
    (tq, lq, hq, tk, lk, hk, tv, lv, hv, norm_train, norm_step) = refs[:11]
    (oq, ok, ov, out_norm) = refs[11:15]
    held = refs[15:26]
    (gains, sums, in_sem, send_sem, recv_sem, peer_send, peer_recv) = refs[26:]
    outs = (oq, ok, ov)
    me, part = lax.axis_index("rows"), lax.axis_index("tp")
    right, left = lax.rem(me + 1, n), lax.rem(me + n - 1, n)
    has_right, has_left = me < n - 1, me > 0

    barrier = pltpu.get_barrier_semaphore()

    def greet(axis, index):
        pl.semaphore_signal(barrier, inc=1, device_id={axis: index}, device_id_type=MESH)

    loads = [
        pltpu.make_async_copy(source, target, in_sem.at[i])
        for i, (source, target) in enumerate(zip(refs[:11], held))
    ]

    @pl.when(has_right)
    def _():
        greet("rows", right)

    @pl.when(has_left)
    def _():
        greet("rows", left)

    for step in range(1, peers):
        greet("tp", lax.rem(part + step, peers))
    for i in (1, 2, 0, 4, 5, 3, 7, 8, 6, 9, 10):
        loads[i].start()

    pieces = []
    for which, out in enumerate(outs):
        height = out.shape[-2]
        width = LANES if height % LANES == 0 else height
        pieces += [(which, start, width) for start in range(0, height, width)]
    norm_piece = len(pieces)

    def view(c, k):
        if c == norm_piece:
            return gains.at[k]
        which, start, width = pieces[c]
        out = outs[which]
        if len(out.shape) == 3:
            return out.at[k, pl.ds(start, width), :]
        return out.at[pl.ds(start, width), pl.ds(pl.multiple_of(k * rows, rows), rows)]

    def hop(c, k, way):
        return pltpu.make_async_remote_copy(
            src_ref=view(c, k),
            dst_ref=view(c, k),
            send_sem=send_sem.at[way, k, c],
            recv_sem=recv_sem.at[k, c],
            device_id={"rows": left if way else right},
            device_id_type=MESH,
        )

    def both_ways(c):
        @pl.when(has_right)
        def _():
            hop(c, me, 0).start()

        @pl.when(has_left)
        def _():
            hop(c, me, 1).start()

    ready = set()

    def merge(c):
        which, start, width = pieces[c]
        train, low, high = held[3 * which : 3 * which + 3]
        if which not in ready:
            ready.add(which)
            for i in (1, 2, 0):
                loads[3 * which + i].wait()
        span = pl.ds(start, width)
        product = lax.dot_general(
            high[:, span], low[...], (((0,), (0,)), ((), ())), preferred_element_type=jnp.float32
        )
        result = train[:, span].T.astype(jnp.float32) + mix_rate * product
        view(c, me)[...] = result.astype(jnp.bfloat16)

    merge(0)
    merge(1)
    pl.semaphore_wait(
        barrier, peers - 1 + has_right.astype(jnp.int32) + has_left.astype(jnp.int32)
    )
    both_ways(0)
    for c in range(2, norm_piece):
        merge(c)
        both_ways(c - 1)
    loads[9].wait()
    loads[10].wait()
    gains[me, part] = held[9][...] + held[10][...]
    both_ways(norm_piece - 1)

    def to_peer(step):
        return pltpu.make_async_remote_copy(
            src_ref=gains.at[me, part],
            dst_ref=gains.at[me, part],
            send_sem=peer_send.at[step],
            recv_sem=peer_recv.at[step],
            device_id={"tp": lax.rem(part + step, peers)},
            device_id_type=MESH,
        )

    for step in range(1, peers):
        to_peer(step).start()
    for step in range(1, peers):
        to_peer(step).wait()
    both_ways(norm_piece)

    def pass_on(step, carry):
        for c in range(norm_piece + 1):

            @pl.when(me - step >= 0)
            def _():
                hop(c, me - step, 0).wait_recv()

                @pl.when(has_right)
                def _():
                    hop(c, me - step, 0).start()

            @pl.when(me + step < n)
            def _():
                hop(c, me + step, 1).wait_recv()

                @pl.when(has_left)
                def _():
                    hop(c, me + step, 1).start()

        return carry

    lax.fori_loop(1, n, pass_on, 0)
    for k in range(n):
        for t in range(peers):
            sums[k * peers + t : k * peers + t + 1, :] = gains[k, t]
    out_norm[...] = sums[...].astype(jnp.bfloat16)

    def sent(step, carry):
        for c in range(norm_piece + 1):

            @pl.when((me - step >= 0) & has_right)
            def _():
                hop(c, me - step, 0).wait_send()

            @pl.when((me + step < n) & has_left)
            def _():
                hop(c, me + step, 1).wait_send()

        return carry

    lax.fori_loop(0, n, sent, 0)


def settle(*refs):
    *arrays, sem = refs
    half = len(arrays) // 2
    copies = [
        pltpu.make_async_copy(source, target, sem.at[i])
        for i, (source, target) in enumerate(zip(arrays[:half], arrays[half:]))
    ]
    for copy in copies:
        copy.start()
    for copy in copies:
        copy.wait()


def solution(mesh):
    n, peers = mesh.shape["rows"], mesh.shape["tp"]

    def shards(tq, lq, hq, tk, lk, hk, tv, lv, hv, norm_train, norm_step):
        rows = tq.shape[0]
        whole_tiles = rows % LANES == 0
        trains = (tq, tk, tv)
        operands = (
            tq, lq.T, hq, tk, lk.T, hk, tv, lv.T, hv,
            norm_train.reshape(1, -1), norm_step.reshape(1, -1),
        )
        heights = [train.shape[1] for train in trains]
        shapes = [
            (height, n * rows) if whole_tiles else (n, height, rows) for height in heights
        ]
        pieces = 1 + sum(h // LANES if h % LANES == 0 else 1 for h in heights)
        width = norm_train.shape[0]
        place = pltpu.VMEM if whole_tiles else jax.ShapeDtypeStruct
        outs = pl.pallas_call(
            functools.partial(kernel, n, peers, rows),
            out_shape=[
                place(shape, jnp.bfloat16) for shape in (*shapes, (n * peers, width))
            ],
            in_specs=[pl.BlockSpec(memory_space=pl.ANY)] * len(operands),
            out_specs=[pl.BlockSpec(memory_space=pltpu.VMEM)] * 4,
            scratch_shapes=[pltpu.VMEM(x.shape, x.dtype) for x in operands]
            + [
                pltpu.VMEM((n, peers, 1, width), jnp.float32),
                pltpu.VMEM((n * peers, width), jnp.float32),
                pltpu.SemaphoreType.DMA((len(operands),)),
                pltpu.SemaphoreType.DMA((2, n, pieces)),
                pltpu.SemaphoreType.DMA((n, pieces)),
                pltpu.SemaphoreType.DMA((peers,)),
                pltpu.SemaphoreType.DMA((peers,)),
            ],
            compiler_params=pltpu.CompilerParams(collective_id=0, has_side_effects=True),
        )(*operands)
        if whole_tiles:
            *finals, norm = pl.pallas_call(
                settle,
                out_shape=[jax.ShapeDtypeStruct(out.shape, out.dtype) for out in outs],
                in_specs=[pl.BlockSpec(memory_space=pltpu.VMEM)] * len(outs),
                out_specs=[pl.BlockSpec(memory_space=pl.ANY)] * len(outs),
                scratch_shapes=[pltpu.SemaphoreType.DMA((len(outs),))],
                compiler_params=pltpu.CompilerParams(vmem_limit_bytes=8 * 1024 * 1024),
            )(*outs)
            return (*finals, norm.reshape(-1))
        finals = [
            out.transpose(1, 0, 2).reshape(height, n * rows)
            for out, height in zip(outs, heights)
        ]
        return (*finals, outs[3].reshape(-1))

    in_specs = (
        P(("unit", "rows"), "tp"),
        P(("unit", "rows"), None),
        P("unit", "tp"),
    ) * 3 + (P(("unit", "rows", "tp")),) * 2
    out_specs = (P(("unit", "tp"), None),) * 3 + (P("unit"),)
    return jax.shard_map(shards, mesh=mesh, in_specs=in_specs, out_specs=out_specs, check_vma=False)
```
